32 devices in a mesh: ctx: 8 (over z, x), kv: 2 (over y), pb: 2 (over core).
Axes of the slice: x: 2, y: 2, z: 4, core: 2. Of those that a mesh axis runs over, the one named last changes fastest.
Arguments:
- queries: bfloat16 [2, 8, 256, 128], P('kv', None, 'pb'), may hold values from -24 to 24
- cache_keys: bfloat16 [2, 32768, 128], P('kv', 'ctx'), may hold values from -6 to 6
- cache_values: bfloat16 [2, 32768, 128], P('kv', 'ctx'), may hold values from -6 to 6
- sel_index: int32 [2, 512], P('kv', 'ctx'), may hold values from 0 to 32767, as said below
Outputs:
- gram: float32 [2, 512, 512], P('kv', ('ctx', 'pb'))
- value_rhs: float32 [2, 512, 128], P('kv', ('ctx', 'pb'))
- mass_gap: float32 [2, 8, 256], P('kv', None, 'pb')
The draws below stay inside these ranges and needn't reach their ends.
Inputs may be any that keep to these rules, and one draw needn't show every extreme that they name: `sel_index`: for every KV head, entries k * 64 to (k + 1) * 64 - 1 are distinct positions of context block k (from k * 4096 to (k + 1) * 4096 - 1), in increasing order.
All inputs are finite; a program needn't handle non-finite values.
Results may differ from the reference program's by a relative error of at most 0.0016.
Values may be sent and summed in bfloat16 or wider, within the bound.
A program may use at most 64 MiB of HBM per device.

```python
import jax
import jax.numpy as jnp
from jax import lax

HD = 128
G = 8
CTX_DEV = 4096
SEL_DEV = 64
KVH = 2
CTX = 32768
SEL = 512
R = 256


def selection(key):
    base = jax.random.fold_in(key, 4099)
    blocks = CTX // CTX_DEV
    subkeys = jax.random.split(base, KVH * blocks)
    picks = jax.vmap(lambda sub: jnp.sort(jax.random.permutation(sub, CTX_DEV)[:SEL_DEV]))(subkeys)
    offsets = jnp.arange(KVH * blocks, dtype=jnp.int32) % blocks * CTX_DEV
    return (picks.astype(jnp.int32) + offsets[:, None]).reshape(KVH, SEL_DEV * blocks).astype(jnp.int32)


def draw_sel_index(key, part):
    return selection(key)


def draw_cache_keys(key, part):
    inner = jax.random.fold_in(key, 17)
    base = jnp.clip(jax.random.normal(inner, (KVH, CTX, HD), jnp.float32), -6.0, 6.0)
    return base.astype(jnp.bfloat16)


def draw_queries(key, part):
    inner = jax.random.fold_in(key, 29)
    base = jnp.clip(jax.random.normal(inner, (KVH, G, R, HD), jnp.float32), -6.0, 6.0)
    return base.astype(jnp.bfloat16)


def steps_of(key, extent, pieces, low, high):
    level, own = 1.0, jax.random.fold_in(key, 6)
    for axis_at, blocks in pieces:
        heights = jnp.exp(jax.random.uniform(jax.random.fold_in(own, axis_at), (blocks,), jnp.float32, low / len(pieces), high / len(pieces)))
        level = level * jnp.repeat(heights, extent[axis_at] // blocks).reshape([-1 if axis == axis_at else 1 for axis in range(len(extent))])
    return level


def gaussian(key, extent, scale, bound, pieces=(), held_as=jnp.bfloat16):
    loudness = steps_of(key, extent, pieces, -0.22, 0.18) if pieces else 1.0
    values = jax.random.normal(key, extent, jnp.float32) * scale * loudness
    return jnp.minimum(jnp.maximum(values, -bound), bound).astype(held_as)


def setup_inputs(seed: int = 0) -> dict:
    seeds = jax.random.split(jax.random.key(seed), 5)
    queries = draw_queries(jax.random.fold_in(seeds[4], 71), 0)
    cache_keys = draw_cache_keys(jax.random.fold_in(seeds[4], 71), 0)
    cache_values = gaussian(seeds[2], (KVH, CTX, HD), 1.0, 6.0, ((0, 2), (1, 8)))
    sel_index = draw_sel_index(jax.random.fold_in(seeds[4], 71), 0)
    return dict(queries=queries, cache_keys=cache_keys, cache_values=cache_values, sel_index=sel_index)


eps = 1e-06

def head_terms(inputs):
    query, keys, values, index = inputs
    width = query.shape[-1]
    scale = width ** (-0.5)
    rows = query.reshape(-1, width)
    blocks = CTX // CTX_DEV
    key_blocks = keys.reshape(blocks, CTX_DEV, width)
    value_blocks = values.reshape(blocks, CTX_DEV, width)

    def one_block(carry, pair):
        key_block, value_block = pair
        scores = jnp.dot(rows, key_block.T, preferred_element_type=jnp.float32) * scale
        block_max = lax.optimization_barrier(jnp.max(scores, axis=1))
        expo = jnp.exp(scores - block_max[:, None])
        block_total = lax.optimization_barrier(jnp.sum(expo, axis=1))
        block_out = jnp.dot(expo.astype(jnp.bfloat16), value_block, preferred_element_type=jnp.float32)
        return (carry, (block_max, block_total, block_out))
    _, (maxima, totals, outs) = lax.scan(one_block, jnp.float32(0.0), (key_blocks, value_blocks))
    top = lax.optimization_barrier(jnp.max(maxima, axis=0))
    weight = jnp.exp(maxima - top[None, :])
    total = lax.optimization_barrier(jnp.sum(weight * totals, axis=0))
    summed = lax.optimization_barrier(jnp.sum(weight[:, :, None] * outs, axis=0))
    target = summed / total[:, None]
    target_y = (target * lax.rsqrt(lax.optimization_barrier(jnp.mean(target * target, axis=1, keepdims=True)) + eps)).astype(jnp.bfloat16)
    compact = jnp.take(keys, index.astype(jnp.int32), axis=0)
    cscores = jnp.dot(rows, compact.T, preferred_element_type=jnp.float32) * scale
    cmax = lax.optimization_barrier(jnp.max(cscores, axis=1))
    cexp = jnp.exp(cscores - cmax[:, None])
    ctotal = lax.optimization_barrier(jnp.sum(cexp, axis=1))
    feat = (SEL * cexp / ctotal[:, None]).astype(jnp.bfloat16)
    inverse = 1.0 / (G * R)
    gram = jnp.dot(feat.T, feat, preferred_element_type=jnp.float32) * inverse
    value_rhs = jnp.dot(feat.T, target_y, preferred_element_type=jnp.float32) * inverse
    mass_gap = (top + jnp.log(total) - (cmax + jnp.log(ctotal))).reshape(G, R)
    return (gram, value_rhs, mass_gap)

def reference(queries, cache_keys, cache_values, sel_index):
    gram, value_rhs, mass_gap = lax.map(head_terms, (queries, cache_keys, cache_values, sel_index))
    return (gram, value_rhs, mass_gap)
```

```python
import functools
import math

import jax
import jax.numpy as jnp
from jax import lax
from jax.experimental import pallas as pl
from jax.experimental.pallas import tpu as pltpu
from jax.sharding import PartitionSpec as P

MESH = pl.DeviceIdType.MESH
eps = 1e-06
f32 = jnp.float32
bf16 = jnp.bfloat16


def dot_nt(a, b):
    return lax.dot_general(a, b, (((1,), (1,)), ((), ())), preferred_element_type=f32)


def fold(x, op):
    rows, cols = x.shape
    return op(x.reshape(rows // 8, 8, cols), axis=0)


def kernel(
    cfg, q_hbm, k_hbm, v_hbm, sel_hbm, gram_ref, rhs_ref, gap_ref,
    q_ref, k_ref, v_ref, sel_ref, vt, scores, comp, both, xrecv, zsend, zrecv, feat, gpart, grecv,
    rpart, precv, rsend, rrecv, in_sem,
    csend_sem, crecv_sem, xsend_sem, xrecv_sem, zsend_sem, zrecv_sem, gsend_sem, grecv_sem,
    psend_sem, precv_sem, rsend_sem, rrecv_sem,
):
    loads = [
        pltpu.make_async_copy(src, dst, in_sem.at[i])
        for i, (src, dst) in enumerate(
            ((sel_hbm, sel_ref), (k_hbm, k_ref), (q_hbm, q_ref), (v_hbm, v_ref))
        )
    ]
    for load in loads:
        load.start()
    n, npb = cfg["n"], cfg["npb"]
    rows, width = q_ref.shape
    keys = k_ref.shape[0]
    sel_dev = sel_ref.shape[1]
    sel_all = n * sel_dev
    piece = sel_dev // npb
    chunk = rows // n
    per = cfg["per"]
    block = per * chunk
    groups = n // per
    scale = width ** (-0.5)
    c2 = scale * math.log2(math.e)
    tile = cfg["tile"]
    inverse = 1.0 / (rows * npb)

    me = lax.axis_index("ctx")
    pb = lax.axis_index("pb")
    my_group = me // per
    my_pair = me // 2
    side = lax.rem(me, 2)

    barrier = pltpu.get_barrier_semaphore()

    def greet(j, carry):
        for d in range(npb):
            @pl.when(jnp.logical_or(j > 0, d > 0))
            def _():
                pl.semaphore_signal(
                    barrier, inc=1,
                    device_id={"ctx": lax.rem(me + j, n), "pb": lax.rem(pb + d, npb)},
                    device_id_type=MESH,
                )
        return carry

    lax.fori_loop(0, n, greet, 0)

    loads[0].wait()
    loads[1].wait()
    pos = (sel_ref[...] - me * keys).astype(f32)
    diag = lax.broadcasted_iota(jnp.int32, (sel_dev, sel_dev), 0) == lax.broadcasted_iota(
        jnp.int32, (sel_dev, sel_dev), 1
    )
    column = jnp.sum(jnp.where(diag, pos, 0.0), axis=1, keepdims=True).astype(jnp.int32)
    picked = jnp.zeros((sel_dev, width), f32)
    for t in range(0, keys, tile):
        hot = (lax.broadcasted_iota(jnp.int32, (sel_dev, tile), 1) + t == column).astype(f32).astype(bf16)
        picked += jnp.dot(hot, k_ref[t : t + tile, :], preferred_element_type=f32)
    comp[me] = picked.astype(bf16)
    loads[3].wait()
    for t in range(0, keys, tile):
        vt[:, t : t + tile] = v_ref[t : t + tile, :].T

    pl.semaphore_wait(barrier, n * npb - 1)

    def comp_copy(j, src):
        return pltpu.make_async_remote_copy(
            src_ref=comp.at[src], dst_ref=comp.at[src],
            send_sem=csend_sem.at[j], recv_sem=crecv_sem.at[src],
            device_id={"ctx": j}, device_id_type=MESH,
        )

    def x_copy(a):
        return pltpu.make_async_remote_copy(
            src_ref=both.at[a, 1 - side], dst_ref=xrecv.at[a],
            send_sem=xsend_sem.at[a], recv_sem=xrecv_sem.at[a],
            device_id={"ctx": me + 1 - 2 * side}, device_id_type=MESH,
        )

    def z_copy(a, src):
        return pltpu.make_async_remote_copy(
            src_ref=zsend.at[a], dst_ref=zrecv.at[src],
            send_sem=zsend_sem.at[a], recv_sem=zrecv_sem.at[src],
            device_id={"ctx": 2 * a + side}, device_id_type=MESH,
        )

    def merge(parts):
        top = parts[0][width : width + 1, :]
        for part in parts[1:]:
            top = jnp.maximum(top, part[width : width + 1, :])
        total, summed = 0.0, 0.0
        for part in parts:
            weight = jnp.exp2((part[width : width + 1, :] - top) * c2)
            total += weight * part[width + 1 : width + 2, :]
            summed += weight * part[:width, :]
        return top, total, summed

    def put(ref, index, top, total, summed):
        ref[index + (slice(0, width),)] = summed
        ref[index + (slice(width, width + 8),)] = jnp.concatenate(
            [top, total, jnp.zeros((6, chunk), f32)], axis=0
        )

    def pass_on(t):
        first = group_of(t) * (per // 2)
        for u in range(per // 2):
            a = first + u
            x_copy(a).wait_recv()
            merged = merge([both[a, side], xrecv[a]])
            if t == groups - 1:
                @pl.when(a == my_pair)
                def _():
                    put(zrecv, (my_pair,), *merged)

                @pl.when(a != my_pair)
                def _():
                    put(zsend, (a,), *merged)
                    z_copy(a, my_pair).start()
            else:
                put(zsend, (a,), *merged)
                z_copy(a, my_pair).start()

    def send_comp(d, carry):
        comp_copy(lax.rem(me + d, n), me).start()
        return carry

    lax.fori_loop(1, n, send_comp, 0)

    def group_of(t):
        return lax.rem(my_group + 1 + t, groups)

    def load_q(t):
        return q_ref[pl.ds(pl.multiple_of(group_of(t) * block, block), block), :]

    def score_tile(t, q, i, top):
        s = dot_nt(k_ref[i : i + tile, :], q)
        scores[t % 2, i : i + tile, :] = s
        part = fold(s, jnp.max)
        return part if top is None else jnp.maximum(top, part)

    loads[2].wait()
    q = load_q(0)
    top = None
    for i in range(0, keys, tile):
        top = score_tile(0, q, i, top)
    for t in range(groups):
        row_max = jnp.max(top, axis=0, keepdims=True)
        shift = row_max * c2
        total = jnp.zeros((8, block), f32)
        acc = jnp.zeros((width, block), f32)
        top = None
        if t + 1 < groups:
            q = load_q(t + 1)
        for i in range(0, keys, tile):
            p = jnp.exp2(scores[t % 2, i : i + tile, :] * c2 - shift)
            total += fold(p, jnp.sum)
            acc += jnp.dot(vt[:, i : i + tile], p.astype(bf16), preferred_element_type=f32)
            if t + 1 < groups:
                top = score_tile(t + 1, q, i, top)
        row_total = jnp.sum(total, axis=0, keepdims=True)
        first = group_of(t) * (per // 2)
        for u in range(per // 2):
            for e in range(2):
                lanes = slice((2 * u + e) * chunk, (2 * u + e + 1) * chunk)
                put(both, (first + u, e), row_max[:, lanes], row_total[:, lanes], acc[:, lanes])
            x_copy(first + u).start()
        if t > 0:
            pass_on(t - 1)

    def wait_comp(d, carry):
        src = lax.rem(me + d, n)
        comp_copy(src, src).wait_recv()
        return carry

    lax.fori_loop(1, n, wait_comp, 0)
    compact = comp[...].reshape(sel_all, width)

    def features(q):
        c = dot_nt(compact, q)
        cmax = jnp.max(c, axis=0, keepdims=True)
        e = jnp.exp2(c * c2 - cmax * c2)
        ctotal = jnp.sum(e, axis=0, keepdims=True)
        return (e * (sel_all / ctotal)).astype(bf16), cmax * scale + jnp.log(ctotal)

    gram = jnp.zeros((sel_dev, sel_all), f32)
    for g in range(groups):
        feat[g] = features(q_ref[g * block : (g + 1) * block, :])[0]
    for g in range(groups):
        own = feat[g, pl.ds(pl.multiple_of(me * sel_dev, sel_dev), sel_dev), :]
        gram += dot_nt(own, feat[g])
    for d in range(npb):
        gpart[d] = gram[d * piece : (d + 1) * piece, :] * inverse

    def g_copy(d, src):
        return pltpu.make_async_remote_copy(
            src_ref=gpart.at[d], dst_ref=grecv.at[src],
            send_sem=gsend_sem.at[d], recv_sem=grecv_sem.at[src],
            device_id={"pb": d}, device_id_type=MESH,
        )

    for d in range(1, npb):
        g_copy(lax.rem(pb + d, npb), pb).start()

    own_feat, own_mass = features(q_ref[pl.ds(pl.multiple_of(me * chunk, chunk), chunk), :])

    pass_on(groups - 1)

    def wait_z(d, carry):
        src = lax.rem(my_pair + d, n // 2)
        z_copy(src, src).wait_recv()
        return carry

    lax.fori_loop(1, n // 2, wait_z, 0)
    top, total, summed = merge([zrecv[b] for b in range(n // 2)])
    target = summed / total
    y = (target * lax.rsqrt(jnp.mean(target * target, axis=0, keepdims=True) + eps)).astype(bf16)
    gap = top * scale + jnp.log(total) - own_mass
    gap8 = jnp.broadcast_to(gap, (8, chunk))
    rhs = dot_nt(own_feat, y) * inverse

    def p_copy(d, src):
        return pltpu.make_async_remote_copy(
            src_ref=rpart.at[d], dst_ref=precv.at[src],
            send_sem=psend_sem.at[d], recv_sem=precv_sem.at[src],
            device_id={"pb": d}, device_id_type=MESH,
        )

    for d in range(npb):
        for j in range(n):
            start = (j * npb + d) * piece
            rpart[d, j] = rhs[start : start + piece, :]
    for d in range(1, npb):
        p_copy(lax.rem(pb + d, npb), pb).start()

    def r_copy(j, src):
        return pltpu.make_async_remote_copy(
            src_ref=rsend.at[j], dst_ref=rrecv.at[src],
            send_sem=rsend_sem.at[j], recv_sem=rrecv_sem.at[src],
            device_id={"ctx": j}, device_id_type=MESH,
        )

    for d in range(1, npb):
        p_copy(pb, lax.rem(pb + d, npb)).wait_recv()
    for j in range(n):
        part = rpart[pb, j]
        for d in range(1, npb):
            part += precv[lax.rem(pb + d, npb), j]
        rsend[j, :piece, :] = part
        rsend[j, piece:, :chunk] = gap8

    def send_r(d, carry):
        r_copy(lax.rem(me + d, n), me).start()
        return carry

    lax.fori_loop(1, n, send_r, 0)
    rrecv[me] = rsend[me]

    for d in range(1, npb):
        g_copy(pb, lax.rem(pb + d, npb)).wait_recv()
    result = gpart[pb]
    for d in range(1, npb):
        result += grecv[lax.rem(pb + d, npb)]
    gram_ref[...] = result
    for d in range(1, npb):
        g_copy(lax.rem(pb + d, npb), pb).wait_send()

    for d in range(1, npb):
        p_copy(lax.rem(pb + d, npb), pb).wait_send()

    def drain(d, carry):
        comp_copy(lax.rem(me + d, n), me).wait_send()
        return carry

    lax.fori_loop(1, n, drain, 0)

    def drain_x(a, carry):
        x_copy(a).wait_send()
        return carry

    lax.fori_loop(0, n // 2, drain_x, 0)

    def drain_z(d, carry):
        z_copy(lax.rem(my_pair + d, n // 2), my_pair).wait_send()
        return carry

    lax.fori_loop(1, n // 2, drain_z, 0)

    def wait_r(d, carry):
        src = lax.rem(me + d, n)
        r_copy(src, src).wait_recv()
        return carry

    lax.fori_loop(1, n, wait_r, 0)
    out = jnp.zeros((piece, width), f32)
    for j in range(n):
        out += rrecv[j, :piece, :]
        gap_ref[j : j + 1, :] = rrecv[j, piece : piece + 1, :chunk]
    rhs_ref[...] = out

    def drain_r(d, carry):
        r_copy(lax.rem(me + d, n), me).wait_send()
        return carry

    lax.fori_loop(1, n, drain_r, 0)


def solution(mesh):
    n, npb = mesh.shape["ctx"], mesh.shape["pb"]

    def shards(queries, cache_keys, cache_values, sel_index):
        heads, rows_dev, width = queries.shape[1:]
        rows = heads * rows_dev
        keys = cache_keys.shape[1]
        sel_dev = sel_index.shape[1]
        sel_all, piece, chunk = sel_dev * n, sel_dev // npb, rows // n
        per = max(2, min(n, 256 // chunk))
        while n % per or per % 2:
            per -= 1
        block = per * chunk
        tile = math.gcd(keys, 512)
        cfg = dict(n=n, npb=npb, per=per, tile=tile)
        vmem = pl.BlockSpec(memory_space=pltpu.VMEM)
        dma = pltpu.SemaphoreType.DMA
        gram, rhs, gap = pl.pallas_call(
            functools.partial(kernel, cfg),
            out_shape=(
                jax.ShapeDtypeStruct((piece, sel_all), f32),
                jax.ShapeDtypeStruct((piece, width), f32),
                jax.ShapeDtypeStruct((n, chunk), f32),
            ),
            in_specs=[pl.BlockSpec(memory_space=pltpu.HBM)] * 4,
            out_specs=(vmem,) * 3,
            scratch_shapes=[
                pltpu.VMEM((rows, width), bf16),
                pltpu.VMEM((keys, width), bf16),
                pltpu.VMEM((keys, width), bf16),
                pltpu.VMEM((1, sel_dev), jnp.int32),
                pltpu.VMEM((width, keys), bf16),
                pltpu.VMEM((2, keys, block), f32),
                pltpu.VMEM((n, sel_dev, width), bf16),
                pltpu.VMEM((n // 2, 2, width + 8, chunk), f32),
                pltpu.VMEM((n // 2, width + 8, chunk), f32),
                pltpu.VMEM((n // 2, width + 8, chunk), f32),
                pltpu.VMEM((n // 2, width + 8, chunk), f32),
                pltpu.VMEM((n // per, sel_all, block), bf16),
                pltpu.VMEM((npb, piece, sel_all), f32),
                pltpu.VMEM((npb, piece, sel_all), f32),
                pltpu.VMEM((npb, n, piece, width), f32),
                pltpu.VMEM((npb, n, piece, width), f32),
                pltpu.VMEM((n, piece + 8, width), f32),
                pltpu.VMEM((n, piece + 8, width), f32),
                dma((4,)),
                dma((n,)), dma((n,)), dma((n // 2,)), dma((n // 2,)), dma((n // 2,)), dma((n // 2,)),
                dma((npb,)), dma((npb,)), dma((npb,)), dma((npb,)), dma((n,)), dma((n,)),
            ],
            compiler_params=pltpu.CompilerParams(
                collective_id=0, has_side_effects=True, vmem_limit_bytes=50 * 1024 * 1024
            ),
        )(*[pltpu.with_memory_space_constraint(a, pltpu.HBM) for a in (queries[0].reshape(rows, width), cache_keys[0], cache_values[0], sel_index)])
        def emit(a_ref, b_ref, c_ref, d_ref, e_ref, f_ref, sems):
            copies = [
                pltpu.make_async_copy(src, dst, sems.at[i])
                for i, (src, dst) in enumerate(((a_ref, d_ref), (b_ref, e_ref), (c_ref, f_ref)))
            ]
            for c in copies:
                c.start()
            for c in copies:
                c.wait()

        gram, rhs, gap = pl.pallas_call(
            emit,
            out_shape=tuple(jax.ShapeDtypeStruct(a.shape, f32) for a in (gram, rhs, gap)),
            in_specs=[pl.BlockSpec(memory_space=pltpu.VMEM)] * 3,
            out_specs=(pl.BlockSpec(memory_space=pltpu.HBM),) * 3,
            scratch_shapes=[dma((3,))],
        )(*[pltpu.with_memory_space_constraint(a, pltpu.VMEM) for a in (gram, rhs, gap)])
        return gram[None], rhs[None], gap.reshape(1, heads, rows_dev)

    in_specs = (
        P("kv", None, "pb", None),
        P("kv", "ctx", None),
        P("kv", "ctx", None),
        P("kv", "ctx"),
    )
    out_specs = (P("kv", ("ctx", "pb"), None), P("kv", ("ctx", "pb"), None), P("kv", None, "pb"))
    return jax.shard_map(shards, mesh=mesh, in_specs=in_specs, out_specs=out_specs, check_vma=False)
```

```python
import functools
import math

import jax
import jax.numpy as jnp
from jax import lax
from jax.experimental import pallas as pl
from jax.experimental.pallas import tpu as pltpu
from jax.sharding import PartitionSpec as P

MESH = pl.DeviceIdType.MESH
eps = 1e-06
ln2 = math.log(2.0)
top16 = 32767.0
f32 = jnp.float32
bf16 = jnp.bfloat16
i16 = jnp.int16


def dot_nt(a, b):
    return lax.dot_general(a, b, (((1,), (1,)), ((), ())), preferred_element_type=f32)


def fold(x, op, height):
    rows, cols = x.shape
    return op(x.reshape(rows // height, height, cols), axis=0)


def encode(x):
    peak = jnp.maximum(jnp.max(jnp.abs(x), axis=0, keepdims=True), 1e-30)
    codes = jnp.floor(x * (top16 / peak) + 0.5)
    return codes.astype(jnp.int32).astype(i16), peak * (1.0 / top16)


def decode(codes, step):
    return codes.astype(jnp.int32).astype(f32) * step


def far_first(i, t, n):
    flip = i // (n // 2)
    low = i + flip * (n - 1 - 2 * i)
    other = n - 1 - t - (low + t) // (n - 1)
    return other + flip * (n - 1 - 2 * other)


def kernel(
    cfg, q_hbm, k_hbm, v_hbm, sel_hbm, gram_ref, rhs_ref, gap_ref,
    q_ref, k_ref, v_ref, sel_ref, vt, sa, sb, acc, comp,
    both, code, cstat, xcode, xstat, zcode, zstat, zrcode, zrstat,
    feat, mass, gpart, grecv, fsend, frecv, ysend, yrecv, rcode, rstat, rrcode, rrstat, in_sem,
    csend_sem, crecv_sem, xsend_sem, xrecv_sem, zsend_sem, zrecv_sem, gsend_sem, grecv_sem,
    fsend_sem, frecv_sem, ysend_sem, yrecv_sem, rsend_sem, rrecv_sem,
):
    loads = [
        pltpu.make_async_copy(src, dst, in_sem.at[i])
        for i, (src, dst) in enumerate(
            ((sel_hbm, sel_ref), (k_hbm, k_ref), (q_hbm, q_ref), (v_hbm, v_ref))
        )
    ]
    for load in loads:
        load.start()
    n, npb = cfg["n"], cfg["npb"]
    rows, width = q_ref.shape
    keys = k_ref.shape[0]
    sel_dev = sel_ref.shape[1]
    sel_all = n * sel_dev
    piece = sel_dev // npb
    chunk = rows // n
    per = cfg["per"]
    block = per * chunk
    groups = n // per
    scale = width ** (-0.5)
    c2 = scale * math.log2(math.e)
    first_tile, tile, height = cfg["first_tile"], cfg["tile"], 32
    inverse = 1.0 / (rows * npb)

    me = lax.axis_index("ctx")
    pb = lax.axis_index("pb")
    my_group = me // per
    my_pair = me // 2
    side = lax.rem(me, 2)

    barrier = pltpu.get_barrier_semaphore()

    def greet(j, carry):
        for d in range(npb):
            @pl.when(jnp.logical_or(j > 0, d > 0))
            def _():
                pl.semaphore_signal(
                    barrier, inc=1,
                    device_id={"ctx": lax.rem(me + j, n), "pb": lax.rem(pb + d, npb)},
                    device_id_type=MESH,
                )
        return carry

    lax.fori_loop(0, n, greet, 0)

    def comp_copy(j, src):
        return pltpu.make_async_remote_copy(
            src_ref=comp.at[src], dst_ref=comp.at[src],
            send_sem=csend_sem.at[j], recv_sem=crecv_sem.at[src],
            device_id={"ctx": j}, device_id_type=MESH,
        )

    def x_copies(a):
        there = {"ctx": me + 1 - 2 * side}
        return [
            pltpu.make_async_remote_copy(
                src_ref=src.at[a, 1 - side], dst_ref=dst.at[a],
                send_sem=xsend_sem.at[i, a], recv_sem=xrecv_sem.at[i, a],
                device_id=there, device_id_type=MESH,
            )
            for i, (src, dst) in enumerate(((code, xcode), (cstat, xstat)))
        ]

    def z_copies(a, src_pair):
        there = {"ctx": 2 * a + side}
        return [
            pltpu.make_async_remote_copy(
                src_ref=src.at[a], dst_ref=dst.at[src_pair],
                send_sem=zsend_sem.at[i, a], recv_sem=zrecv_sem.at[i, src_pair],
                device_id=there, device_id_type=MESH,
            )
            for i, (src, dst) in enumerate(((zcode, zrcode), (zstat, zrstat)))
        ]

    def pb_copy(send, recv, send_sem, recv_sem, d, src):
        return pltpu.make_async_remote_copy(
            src_ref=send.at[d], dst_ref=recv.at[src],
            send_sem=send_sem.at[d], recv_sem=recv_sem.at[src],
            device_id={"pb": d}, device_id_type=MESH,
        )

    def g_copy(d, src):
        return pb_copy(gpart, grecv, gsend_sem, grecv_sem, d, src)

    def f_copy(d, src):
        return pb_copy(fsend, frecv, fsend_sem, frecv_sem, d, src)

    def y_copy(d, src):
        return pltpu.make_async_remote_copy(
            src_ref=ysend, dst_ref=yrecv.at[src],
            send_sem=ysend_sem.at[d], recv_sem=yrecv_sem.at[src],
            device_id={"pb": d}, device_id_type=MESH,
        )

    def r_copies(j, src_ctx):
        return [
            pltpu.make_async_remote_copy(
                src_ref=src.at[j], dst_ref=dst.at[src_ctx],
                send_sem=rsend_sem.at[i, j], recv_sem=rrecv_sem.at[i, src_ctx],
                device_id={"ctx": j}, device_id_type=MESH,
            )
            for i, (src, dst) in enumerate(((rcode, rrcode), (rstat, rrstat)))
        ]

    def stats(top, total, step):
        return jnp.concatenate([top, total, step, jnp.zeros((5, top.shape[1]), f32)], axis=0)

    def merge(parts):
        top = parts[0][1][0:1, :]
        for _, stat in parts[1:]:
            top = jnp.maximum(top, stat[0:1, :])
        total, summed = 0.0, 0.0
        for part, stat in parts:
            weight = jnp.exp2(stat[0:1, :] - top)
            total += weight * stat[1:2, :]
            summed += weight * part()
        return top, total, summed

    def pass_on(t):
        first = group_of(t) * (per // 2)
        for u in range(per // 2):
            a = first + u
            for copy in x_copies(a):
                copy.wait_recv()
            theirs, ours = xstat[a], cstat[a, side]
            top, total, summed = merge([
                (lambda: both[a, side], ours),
                (lambda: decode(xcode[a], theirs[2:3, :]), theirs),
            ])
            codes, step = encode(summed)
            line = stats(top, total, step)
            if t == groups - 1:
                @pl.when(a == my_pair)
                def _():
                    zrcode[my_pair] = codes
                    zrstat[my_pair] = line

                @pl.when(a != my_pair)
                def _():
                    zcode[a] = codes
                    zstat[a] = line
                    for copy in z_copies(a, my_pair):
                        copy.start()
            else:
                zcode[a] = codes
                zstat[a] = line
                for copy in z_copies(a, my_pair):
                    copy.start()

    def group_of(t):
        return my_group if t == groups - 1 else far_first(my_group, t, groups)

    def load_q(t):
        q = q_ref[pl.ds(pl.multiple_of(group_of(t) * block, block), block), :].astype(f32) * c2
        high = q.astype(bf16)
        return jnp.concatenate([high, (q - high.astype(f32)).astype(bf16)], axis=1)

    def at(i, size):
        return pl.ds(pl.multiple_of(i * size, size), size)

    def score_tile(buf, q, where, top):
        k = k_ref[where, :]
        s = dot_nt(jnp.concatenate([k, k], axis=1), q)
        buf[where, :] = s
        return jnp.maximum(top, fold(s, jnp.max, height))

    def send_comp(t, carry):
        comp_copy(far_first(me, t, n), me).start()
        return carry

    lowest = jnp.full((height, block), -jnp.inf, f32)
    with jax.named_scope("w_k"):
        for load in loads[:3]:
            load.wait()
    pos = (sel_ref[...] - me * keys).astype(f32)
    diag = lax.broadcasted_iota(jnp.int32, (sel_dev, sel_dev), 0) == lax.broadcasted_iota(
        jnp.int32, (sel_dev, sel_dev), 1
    )
    column = jnp.sum(jnp.where(diag, pos, 0.0), axis=1, keepdims=True).astype(jnp.int32)
    q = load_q(0)

    def first_scores(i, carry):
        top, picked = carry
        where = at(i, first_tile)
        top = score_tile(sa, q, where, top)
        hot = lax.broadcasted_iota(jnp.int32, (sel_dev, first_tile), 1) == column - i * first_tile
        picked += jnp.dot(hot.astype(f32).astype(bf16), k_ref[where, :], preferred_element_type=f32)
        return top, picked

    top, picked = lax.fori_loop(
        0, keys // first_tile, first_scores, (lowest, jnp.zeros((sel_dev, width), f32))
    )
    comp[me] = picked.astype(bf16)
    with jax.named_scope("w_v"):
        loads[3].wait()

    for t in range(groups):
        row_max = jnp.max(top, axis=0, keepdims=True)
        shift = jnp.broadcast_to(row_max, (8, block))
        now, later = (sa, sb) if t % 2 == 0 else (sb, sa)
        q = load_q(t + 1) if t + 1 < groups else None
        acc[...] = jnp.zeros((width, block), f32)

        def body(i, carry, t=t, q=q, shift=shift, now=now, later=later):
            top, total = carry
            where = at(i, tile)
            x = now[where, :].reshape(tile // 8, 8, block) - shift[None]
            p = jnp.exp2(x).reshape(tile, block)
            total += fold(p, jnp.sum, height)
            if t == 0:
                v = v_ref[where, :].T
                vt[:, where] = v
            else:
                v = vt[:, where]
            acc[...] += jnp.dot(v, p.astype(bf16), preferred_element_type=f32)
            if t + 1 < groups:
                top = score_tile(later, q, where, top)
            return top, total

        top, total = lax.fori_loop(
            0, keys // tile, body, (lowest, jnp.zeros((height, block), f32))
        )
        row_total = jnp.sum(total, axis=0, keepdims=True)
        first = group_of(t) * (per // 2)
        for u in range(per // 2):
            for e in range(2):
                lanes = slice((2 * u + e) * chunk, (2 * u + e + 1) * chunk)
                part = acc[:, lanes]
                codes, step = encode(part)
                both[first + u, e] = part
                code[first + u, e] = codes
                cstat[first + u, e] = stats(row_max[:, lanes], row_total[:, lanes], step)
        if t == 0:
            with jax.named_scope("w_bar"):
                pl.semaphore_wait(barrier, n * npb - 1)
        for u in range(per // 2):
            for copy in x_copies(first + u):
                copy.start()
        if t == 0:
            lax.fori_loop(0, n - 1, send_comp, 0)
        if t > 1:
            with jax.named_scope("pass%d" % (t - 2)):
                pass_on(t - 2)

    def wait_comp(d, carry):
        src = lax.rem(me + d, n)
        comp_copy(src, src).wait_recv()
        return carry

    with jax.named_scope("w_comp"):
        lax.fori_loop(1, n, wait_comp, 0)

    def features(g):
        compact = comp[...].reshape(sel_all, width)
        c = dot_nt(compact, q_ref[g * block : (g + 1) * block, :])
        cmax = jnp.max(c, axis=0, keepdims=True)
        e = jnp.exp2(c * c2 - cmax * c2)
        ctotal = jnp.sum(e, axis=0, keepdims=True)
        f = (e * (sel_all / ctotal)).astype(bf16)
        line = jnp.broadcast_to(cmax * scale + jnp.log(ctotal), (8, block))
        for u in range(per):
            feat[g * per + u] = f[:, u * chunk : (u + 1) * chunk]
            mass[g * per + u] = line[:, u * chunk : (u + 1) * chunk]

    with jax.named_scope("features"):
        for g in range(groups):
            features(g)
    if groups > 1:
        with jax.named_scope("pass%d" % (groups - 2)):
            pass_on(groups - 2)

    for d in range(npb):
        for j in range(n):
            start = (j * npb + d) * piece
            fsend[d, j * piece : (j + 1) * piece, :] = feat[me, start : start + piece, :]
    for d in range(1, npb):
        f_copy(lax.rem(pb + d, npb), pb).start()

    with jax.named_scope("gram"):
        gram = jnp.zeros((sel_dev, sel_all), f32)
        own = pl.ds(pl.multiple_of(me * sel_dev, sel_dev), sel_dev)
        for c in range(n):
            gram += dot_nt(feat[c, own, :], feat[c])
    for d in range(npb):
        gpart[d] = gram[d * piece : (d + 1) * piece, :] * inverse
    for d in range(1, npb):
        g_copy(lax.rem(pb + d, npb), pb).start()

    with jax.named_scope("pass%d" % (groups - 1)):
        pass_on(groups - 1)

    def wait_z(d, carry):
        src = lax.rem(my_pair + d, n // 2)
        for copy in z_copies(src, src):
            copy.wait_recv()
        return carry

    with jax.named_scope("w_z"):
        lax.fori_loop(1, n // 2, wait_z, 0)
    lines = [zrstat[b] for b in range(n // 2)]
    top, total, summed = merge([
        (lambda b=b: decode(zrcode[b], lines[b][2:3, :]), lines[b]) for b in range(n // 2)
    ])
    target = summed / total
    y = (target * lax.rsqrt(jnp.mean(target * target, axis=0, keepdims=True) + eps)).astype(bf16)
    ysend[...] = y
    for d in range(1, npb):
        y_copy(lax.rem(pb + d, npb), pb).start()
    gap = top * ln2 + jnp.log(total) - mass[me, 0:1, :]
    rhs = dot_nt(fsend[pb], y)
    for d in range(1, npb):
        src = lax.rem(pb + d, npb)
        with jax.named_scope("w_y"):
            f_copy(pb, src).wait_recv()
            y_copy(pb, src).wait_recv()
        rhs += dot_nt(frecv[src], yrecv[src])
    rhs = rhs * inverse
    for j in range(n):
        codes, step = encode(rhs[j * piece : (j + 1) * piece, :])
        rcode[j] = codes
        rstat[j, 0:1, :width] = step
        rstat[j, 1:2, :chunk] = gap

    def send_r(t, carry):
        for copy in r_copies(far_first(me, t, n), me):
            copy.start()
        return carry

    lax.fori_loop(0, n - 1, send_r, 0)
    rrcode[me] = rcode[me]
    rrstat[me] = rstat[me]

    with jax.named_scope("w_g"):
        for d in range(1, npb):
            g_copy(pb, lax.rem(pb + d, npb)).wait_recv()
    result = gpart[pb]
    for d in range(1, npb):
        result += grecv[lax.rem(pb + d, npb)]
    gram_ref[...] = result

    for d in range(1, npb):
        there = lax.rem(pb + d, npb)
        for copy in (g_copy, f_copy, y_copy):
            copy(there, pb).wait_send()

    def drain(d, carry):
        comp_copy(lax.rem(me + d, n), me).wait_send()
        return carry

    lax.fori_loop(1, n, drain, 0)

    def drain_x(a, carry):
        for copy in x_copies(a):
            copy.wait_send()
        return carry

    lax.fori_loop(0, n // 2, drain_x, 0)

    def drain_z(d, carry):
        for copy in z_copies(lax.rem(my_pair + d, n // 2), my_pair):
            copy.wait_send()
        return carry

    lax.fori_loop(1, n // 2, drain_z, 0)

    def wait_r(d, carry):
        src = lax.rem(me + d, n)
        for copy in r_copies(src, src):
            copy.wait_recv()
        return carry

    with jax.named_scope("w_r"):
        lax.fori_loop(1, n, wait_r, 0)
    out = jnp.zeros((piece, width), f32)
    for j in range(n):
        out += decode(rrcode[j], rrstat[j, 0:1, :width])
        gap_ref[j : j + 1, :] = rrstat[j, 1:2, :chunk]
    rhs_ref[...] = out

    def drain_r(d, carry):
        for copy in r_copies(lax.rem(me + d, n), me):
            copy.wait_send()
        return carry

    lax.fori_loop(1, n, drain_r, 0)


def emit(*refs):
    count = (len(refs) - 1) // 2
    copies = [pltpu.make_async_copy(refs[i], refs[count + i], refs[-1].at[i]) for i in range(count)]
    for copy in copies:
        copy.start()
    for copy in copies:
        copy.wait()


def solution(mesh):
    n, npb = mesh.shape["ctx"], mesh.shape["pb"]

    def shards(queries, cache_keys, cache_values, sel_index):
        heads, rows_dev, width = queries.shape[1:]
        rows = heads * rows_dev
        keys = cache_keys.shape[1]
        sel_dev = sel_index.shape[1]
        sel_all, piece, chunk = sel_dev * n, sel_dev // npb, rows // n
        per = max(2, min(n, 256 // chunk))
        while n % per or per % 2:
            per -= 1
        block = per * chunk
        cfg = dict(n=n, npb=npb, per=per, first_tile=math.gcd(keys, 1024), tile=math.gcd(keys, 2048))
        lanes = max(width, chunk)
        pairs = n // 2
        vmem = pl.BlockSpec(memory_space=pltpu.VMEM)
        hbm = pl.BlockSpec(memory_space=pltpu.HBM)
        dma = pltpu.SemaphoreType.DMA
        results = (
            jax.ShapeDtypeStruct((piece, sel_all), f32),
            jax.ShapeDtypeStruct((piece, width), f32),
            jax.ShapeDtypeStruct((n, chunk), f32),
        )
        operands = (queries[0].reshape(rows, width), cache_keys[0], cache_values[0], sel_index)
        parts = pl.pallas_call(
            functools.partial(kernel, cfg),
            out_shape=results,
            in_specs=[hbm] * 4,
            out_specs=(vmem,) * 3,
            scratch_shapes=[
                pltpu.VMEM((rows, width), bf16),
                pltpu.VMEM((keys, width), bf16),
                pltpu.VMEM((keys, width), bf16),
                pltpu.VMEM((1, sel_dev), jnp.int32),
                pltpu.VMEM((width, keys), bf16),
                pltpu.VMEM((keys, block), f32),
                pltpu.VMEM((keys, block), f32),
                pltpu.VMEM((width, block), f32),
                pltpu.VMEM((n, sel_dev, width), bf16),
                pltpu.VMEM((pairs, 2, width, chunk), f32),
                pltpu.VMEM((pairs, 2, width, chunk), i16),
                pltpu.VMEM((pairs, 2, 8, chunk), f32),
                pltpu.VMEM((pairs, width, chunk), i16),
                pltpu.VMEM((pairs, 8, chunk), f32),
                pltpu.VMEM((pairs, width, chunk), i16),
                pltpu.VMEM((pairs, 8, chunk), f32),
                pltpu.VMEM((pairs, width, chunk), i16),
                pltpu.VMEM((pairs, 8, chunk), f32),
                pltpu.VMEM((n, sel_all, chunk), bf16),
                pltpu.VMEM((n, 8, chunk), f32),
                pltpu.VMEM((npb, piece, sel_all), f32),
                pltpu.VMEM((npb, piece, sel_all), f32),
                pltpu.VMEM((npb, n * piece, chunk), bf16),
                pltpu.VMEM((npb, n * piece, chunk), bf16),
                pltpu.VMEM((width, chunk), bf16),
                pltpu.VMEM((npb, width, chunk), bf16),
                pltpu.VMEM((n, piece, width), i16),
                pltpu.VMEM((n, 2, lanes), f32),
                pltpu.VMEM((n, piece, width), i16),
                pltpu.VMEM((n, 2, lanes), f32),
                dma((4,)),
                dma((n,)), dma((n,)), dma((2, pairs)), dma((2, pairs)), dma((2, pairs)), dma((2, pairs)),
                dma((npb,)), dma((npb,)), dma((npb,)), dma((npb,)), dma((npb,)), dma((npb,)),
                dma((2, n)), dma((2, n)),
            ],
            compiler_params=pltpu.CompilerParams(
                collective_id=0, has_side_effects=True, vmem_limit_bytes=50 * 1024 * 1024
            ),
        )(*[pltpu.with_memory_space_constraint(a, pltpu.HBM) for a in operands])
        gram, rhs, gap = pl.pallas_call(
            emit,
            out_shape=results,
            in_specs=[vmem] * 3,
            out_specs=(hbm,) * 3,
            scratch_shapes=[dma((3,))],
        )(*[pltpu.with_memory_space_constraint(a, pltpu.VMEM) for a in parts])
        return gram[None], rhs[None], gap.reshape(1, heads, rows_dev)

    in_specs = (
        P("kv", None, "pb", None),
        P("kv", "ctx", None),
        P("kv", "ctx", None),
        P("kv", "ctx"),
    )
    out_specs = (P("kv", ("ctx", "pb"), None), P("kv", ("ctx", "pb"), None), P("kv", None, "pb"))
    return jax.shard_map(shards, mesh=mesh, in_specs=in_specs, out_specs=out_specs, check_vma=False)
```

```python
import functools
import math

import jax
import jax.numpy as jnp
from jax import lax
from jax.experimental import pallas as pl
from jax.experimental.pallas import tpu as pltpu
from jax.sharding import PartitionSpec as P

MESH = pl.DeviceIdType.MESH
eps = 1e-06
ln2 = math.log(2.0)
top16 = 32767.0
f32 = jnp.float32
bf16 = jnp.bfloat16
i16 = jnp.int16


def dot_nt(a, b):
    return lax.dot_general(a, b, (((1,), (1,)), ((), ())), preferred_element_type=f32)


def fold(x, op, height):
    rows, cols = x.shape
    return op(x.reshape(rows // height, height, cols), axis=0)


def encode(x):
    peak = jnp.maximum(jnp.max(jnp.abs(x), axis=0, keepdims=True), 1e-30)
    codes = jnp.floor(x * (top16 / peak) + 0.5)
    return codes.astype(jnp.int32).astype(i16), peak * (1.0 / top16)


def decode(codes, step):
    return codes.astype(jnp.int32).astype(f32) * step


def far_first(i, t, n):
    flip = i // (n // 2)
    low = i + flip * (n - 1 - 2 * i)
    other = n - 1 - t - (low + t) // (n - 1)
    return other + flip * (n - 1 - 2 * other)


def kernel(
    cfg, q_hbm, k_hbm, v_hbm, sel_hbm, gram_ref, rhs_ref, gap_ref,
    q_ref, k_ref, v_ref, sel_ref, vt, sa, sb, acc, comp,
    both, code, cstat, xcode, xstat, zcode, zstat, zrcode, zrstat,
    feat, mass, gpart, grecv, fsend, frecv, ysend, yrecv, rcode, rstat, rrcode, rrstat, in_sem,
    csend_sem, crecv_sem, xsend_sem, xrecv_sem, zsend_sem, zrecv_sem,
    gsend_sem, grecv_sem, fsend_sem, frecv_sem, ysend_sem, yrecv_sem, rsend_sem, rrecv_sem,
):
    loads = [
        pltpu.make_async_copy(src, dst, in_sem.at[i])
        for i, (src, dst) in enumerate(
            ((sel_hbm, sel_ref), (k_hbm, k_ref), (q_hbm, q_ref), (v_hbm, v_ref))
        )
    ]
    for load in loads:
        load.start()
    n, npb = cfg["n"], cfg["npb"]
    rows, width = q_ref.shape
    keys = k_ref.shape[0]
    sel_dev = sel_ref.shape[1]
    sel_all = n * sel_dev
    piece = sel_dev // npb
    chunk = rows // n
    per = cfg["per"]
    block = per * chunk
    groups = n // per
    scale = width ** (-0.5)
    c2 = scale * math.log2(math.e)
    tile, height = cfg["tile"], 32
    inverse = 1.0 / (rows * npb)

    me = lax.axis_index("ctx")
    pb = lax.axis_index("pb")
    my_group = me // per
    my_pair = me // 2
    side = lax.rem(me, 2)

    barrier = pltpu.get_barrier_semaphore()

    def greet(j, carry):
        for d in range(npb):
            @pl.when(jnp.logical_or(j > 0, d > 0))
            def _():
                pl.semaphore_signal(
                    barrier, inc=1,
                    device_id={"ctx": lax.rem(me + j, n), "pb": lax.rem(pb + d, npb)},
                    device_id_type=MESH,
                )
        return carry

    lax.fori_loop(0, n, greet, 0)

    def comp_copy(j):
        return pltpu.make_async_remote_copy(
            src_ref=comp.at[me], dst_ref=comp.at[me],
            send_sem=csend_sem, recv_sem=crecv_sem,
            device_id={"ctx": j}, device_id_type=MESH,
        )

    def all_comp():
        slots = comp.at[pl.ds(0, n - 1)]
        return pltpu.make_async_remote_copy(
            src_ref=slots, dst_ref=slots, send_sem=csend_sem, recv_sem=crecv_sem,
            device_id={"ctx": me}, device_id_type=MESH,
        )

    def x_copies(a):
        there = {"ctx": me + 1 - 2 * side}
        return [
            pltpu.make_async_remote_copy(
                src_ref=src.at[a, 1 - side], dst_ref=dst.at[a],
                send_sem=xsend_sem.at[i], recv_sem=xrecv_sem.at[i, a],
                device_id=there, device_id_type=MESH,
            )
            for i, (src, dst) in enumerate(((code, xcode), (cstat, xstat)))
        ]

    def z_copies(a):
        there = {"ctx": 2 * a + side}
        return [
            pltpu.make_async_remote_copy(
                src_ref=src.at[a], dst_ref=dst.at[my_pair],
                send_sem=zsend_sem.at[i], recv_sem=zrecv_sem.at[i],
                device_id=there, device_id_type=MESH,
            )
            for i, (src, dst) in enumerate(((zcode, zrcode), (zstat, zrstat)))
        ]

    def r_copies(j):
        return [
            pltpu.make_async_remote_copy(
                src_ref=src.at[j], dst_ref=dst.at[me],
                send_sem=rsend_sem.at[i], recv_sem=rrecv_sem.at[i],
                device_id={"ctx": j}, device_id_type=MESH,
            )
            for i, (src, dst) in enumerate(((rcode, rrcode), (rstat, rrstat)))
        ]

    def together(pairs, send_sem, recv_sem, count):
        return [
            pltpu.make_async_remote_copy(
                src_ref=src.at[pl.ds(0, count)], dst_ref=dst.at[pl.ds(0, count)],
                send_sem=send_sem.at[i], recv_sem=recv_sem.at[i],
                device_id={"ctx": me}, device_id_type=MESH,
            )
            for i, (src, dst) in enumerate(pairs)
        ]

    def all_z():
        return together(((zcode, zrcode), (zstat, zrstat)), zsend_sem, zrecv_sem, n // 2 - 1)

    def all_r():
        return together(((rcode, rrcode), (rstat, rrstat)), rsend_sem, rrecv_sem, n - 1)

    def all_x():
        return [
            pltpu.make_async_remote_copy(
                src_ref=src.at[:, 0], dst_ref=src.at[:, 0],
                send_sem=xsend_sem.at[i], recv_sem=xrecv_sem.at[i, 0],
                device_id={"ctx": me}, device_id_type=MESH,
            )
            for i, src in enumerate((code, cstat))
        ]

    def pb_copy(send, recv, send_sem, recv_sem, d, src):
        return pltpu.make_async_remote_copy(
            src_ref=send.at[d], dst_ref=recv.at[src],
            send_sem=send_sem.at[d], recv_sem=recv_sem.at[src],
            device_id={"pb": d}, device_id_type=MESH,
        )

    def g_copy(d, src):
        return pb_copy(gpart, grecv, gsend_sem, grecv_sem, d, src)

    def f_copy(d, src):
        return pb_copy(fsend, frecv, fsend_sem, frecv_sem, d, src)

    def y_copy(d, src):
        return pltpu.make_async_remote_copy(
            src_ref=ysend, dst_ref=yrecv.at[src],
            send_sem=ysend_sem.at[d], recv_sem=yrecv_sem.at[src],
            device_id={"pb": d}, device_id_type=MESH,
        )

    def stats(top, total, step):
        return jnp.concatenate([top, total, step, jnp.zeros((5, top.shape[1]), f32)], axis=0)

    def merge(parts):
        top = parts[0][1][0:1, :]
        for _, stat in parts[1:]:
            top = jnp.maximum(top, stat[0:1, :])
        total, summed = 0.0, 0.0
        for part, stat in parts:
            weight = jnp.exp2(stat[0:1, :] - top)
            total += weight * stat[1:2, :]
            summed += weight * part()
        return top, total, summed

    def pass_on(t):
        first = group_of(t) * (per // 2)
        for u in range(per // 2):
            a = first + u
            for copy in x_copies(a):
                copy.wait_recv()
            theirs, ours = xstat[a], cstat[a, side]
            top, total, summed = merge([
                (lambda: both[a, side], ours),
                (lambda: decode(xcode[a], theirs[2:3, :]), theirs),
            ])
            codes, step = encode(summed)
            line = stats(top, total, step)
            if t == groups - 1:
                @pl.when(a == my_pair)
                def _():
                    zrcode[my_pair] = codes
                    zrstat[my_pair] = line

                @pl.when(a != my_pair)
                def _():
                    zcode[a] = codes
                    zstat[a] = line
                    for copy in z_copies(a):
                        copy.start()
            else:
                zcode[a] = codes
                zstat[a] = line
                for copy in z_copies(a):
                    copy.start()

    def group_of(t):
        return my_group if t == groups - 1 else far_first(my_group, t, groups)

    def load_q(t):
        q = q_ref[pl.ds(pl.multiple_of(group_of(t) * block, block), block), :].astype(f32) * c2
        high = q.astype(bf16)
        return jnp.concatenate([high, (q - high.astype(f32)).astype(bf16)], axis=1)

    def at(i, size):
        return pl.ds(pl.multiple_of(i * size, size), size)

    def score_tile(buf, q, where, top):
        k = k_ref[where, :]
        s = dot_nt(jnp.concatenate([k, k], axis=1), q)
        buf[where, :] = s
        return jnp.maximum(top, fold(s, jnp.max, height))

    lowest = jnp.full((height, block), -jnp.inf, f32)

    def first_scores():
        q, column = load_q(0), column_of()

        def body(i, carry):
            top, picked = carry
            where = at(i, tile)
            top = score_tile(sa, q, where, top)
            hot = lax.broadcasted_iota(jnp.int32, (sel_dev, tile), 1) == column - i * tile
            picked += jnp.dot(hot.astype(f32).astype(bf16), k_ref[where, :], preferred_element_type=f32)
            return top, picked

        start = (lowest, jnp.zeros((sel_dev, width), f32))
        top, picked = lax.fori_loop(0, keys // tile, body, start)
        comp[me] = picked.astype(bf16)
        return top

    def attend(t, top):
        shift = jnp.broadcast_to(jnp.max(top, axis=0, keepdims=True), (8, block))
        now, later = (sa, sb) if t % 2 == 0 else (sb, sa)
        q = load_q(t + 1) if t + 1 < groups else None
        acc[...] = jnp.zeros((width, block), f32)

        def body(i, carry):
            top, total = carry
            where = at(i, tile)
            x = now[where, :].reshape(tile // 8, 8, block) - shift[None]
            p = jnp.exp2(x).reshape(tile, block)
            total += fold(p, jnp.sum, height)
            if t == 0:
                v = v_ref[where, :].T
                vt[:, where] = v
            else:
                v = vt[:, where]
            acc[...] += jnp.dot(v, p.astype(bf16), preferred_element_type=f32)
            if t + 1 < groups:
                top = score_tile(later, q, where, top)
            return top, total

        top, total = lax.fori_loop(
            0, keys // tile, body, (lowest, jnp.zeros((height, block), f32))
        )
        return top, jnp.sum(total, axis=0, keepdims=True), acc[...]

    def send_comp(t, carry):
        comp_copy(far_first(me, t, n)).start()
        return carry

    def column_of():
        pos = (sel_ref[...] - me * keys).astype(f32)
        diag = lax.broadcasted_iota(jnp.int32, (sel_dev, sel_dev), 0) == lax.broadcasted_iota(
            jnp.int32, (sel_dev, sel_dev), 1
        )
        return jnp.sum(jnp.where(diag, pos, 0.0), axis=1, keepdims=True).astype(jnp.int32)

    with jax.named_scope("w_k"):
        for load in loads[:3]:
            load.wait()
    late = my_group == groups - 1

    def open_sends():
        pl.semaphore_wait(barrier, n * npb - 1)

    def start_comp():
        lax.fori_loop(0, n - 1, send_comp, 0)

    top = first_scores()

    @pl.when(late)
    def _():
        with jax.named_scope("w_bar_late"):
            open_sends()
        start_comp()

    with jax.named_scope("w_v"):
        loads[3].wait()

    for t in range(groups):
        row_max = jnp.max(top, axis=0, keepdims=True)
        top, row_total, summed = attend(t, top)
        first = group_of(t) * (per // 2)
        for u in range(per // 2):
            for e in range(2):
                lanes = slice((2 * u + e) * chunk, (2 * u + e + 1) * chunk)
                part = summed[:, lanes]
                codes, step = encode(part)
                both[first + u, e] = part
                code[first + u, e] = codes
                cstat[first + u, e] = stats(row_max[:, lanes], row_total[:, lanes], step)
        if t == 0:
            @pl.when(jnp.logical_not(late))
            def _():
                with jax.named_scope("w_bar"):
                    open_sends()

        for u in range(per // 2):
            for copy in x_copies(first + u):
                copy.start()
        if t == 0:
            pl.when(jnp.logical_not(late))(start_comp)

    for t in range(groups - 2):
        with jax.named_scope("pass%d" % t):
            pass_on(t)
    with jax.named_scope("w_comp"):
        all_comp().wait_recv()

    def features(g):
        compact = comp[...].reshape(sel_all, width)
        c = dot_nt(compact, q_ref[g * block : (g + 1) * block, :])
        cmax = jnp.max(c, axis=0, keepdims=True)
        e = jnp.exp2(c * c2 - cmax * c2)
        ctotal = jnp.sum(e, axis=0, keepdims=True)
        f = (e * (sel_all / ctotal)).astype(bf16)
        line = jnp.broadcast_to(cmax * scale + jnp.log(ctotal), (8, block))
        for u in range(per):
            feat[g * per + u] = f[:, u * chunk : (u + 1) * chunk]
            mass[g * per + u] = line[:, u * chunk : (u + 1) * chunk]

    with jax.named_scope("features"):
        for g in range(groups):
            features(g)
    if groups > 1:
        with jax.named_scope("pass%d" % (groups - 2)):
            pass_on(groups - 2)

    for d in range(npb):
        for j in range(n):
            start = (j * npb + d) * piece
            fsend[d, j * piece : (j + 1) * piece, :] = feat[me, start : start + piece, :]
    for d in range(1, npb):
        f_copy(lax.rem(pb + d, npb), pb).start()

    with jax.named_scope("gram"):
        gram = jnp.zeros((sel_dev, sel_all), f32)
        own = pl.ds(pl.multiple_of(me * sel_dev, sel_dev), sel_dev)
        for c in range(n):
            gram += dot_nt(feat[c, own, :], feat[c])
    for d in range(npb):
        gpart[d] = gram[d * piece : (d + 1) * piece, :] * inverse
    for d in range(1, npb):
        g_copy(lax.rem(pb + d, npb), pb).start()

    with jax.named_scope("pass%d" % (groups - 1)):
        pass_on(groups - 1)

    with jax.named_scope("w_z"):
        for copy in all_z():
            copy.wait_recv()
    lines = [zrstat[b] for b in range(n // 2)]
    top, total, summed = merge([
        (lambda b=b: decode(zrcode[b], lines[b][2:3, :]), lines[b]) for b in range(n // 2)
    ])
    target = summed / total
    y = (target * lax.rsqrt(jnp.mean(target * target, axis=0, keepdims=True) + eps)).astype(bf16)
    ysend[...] = y
    for d in range(1, npb):
        y_copy(lax.rem(pb + d, npb), pb).start()
    gap = top * ln2 + jnp.log(total) - mass[me, 0:1, :]
    rhs = dot_nt(fsend[pb], y)
    for d in range(1, npb):
        src = lax.rem(pb + d, npb)
        with jax.named_scope("w_y"):
            f_copy(pb, src).wait_recv()
            y_copy(pb, src).wait_recv()
        rhs += dot_nt(frecv[src], yrecv[src])
    rhs = rhs * inverse
    for j in range(n):
        codes, step = encode(rhs[j * piece : (j + 1) * piece, :])
        rcode[j] = codes
        rstat[j, 0:1, :width] = step
        rstat[j, 1:2, :chunk] = gap

    def send_r(t, carry):
        for copy in r_copies(far_first(me, t, n)):
            copy.start()
        return carry

    lax.fori_loop(0, n - 1, send_r, 0)
    rrcode[me] = rcode[me]
    rrstat[me] = rstat[me]

    with jax.named_scope("w_g"):
        for d in range(1, npb):
            g_copy(pb, lax.rem(pb + d, npb)).wait_recv()
    result = gpart[pb]
    for d in range(1, npb):
        result += grecv[lax.rem(pb + d, npb)]
    gram_ref[...] = result

    for d in range(1, npb):
        there = lax.rem(pb + d, npb)
        for copy in (g_copy, f_copy, y_copy):
            copy(there, pb).wait_send()
    all_comp().wait_send()
    for copy in all_x() + all_z():
        copy.wait_send()

    with jax.named_scope("w_r"):
        for copy in all_r():
            copy.wait_recv()
    out = jnp.zeros((piece, width), f32)
    for j in range(n):
        out += decode(rrcode[j], rrstat[j, 0:1, :width])
        gap_ref[j : j + 1, :] = rrstat[j, 1:2, :chunk]
    rhs_ref[...] = out

    for copy in all_r():
        copy.wait_send()


def emit(*refs):
    count = (len(refs) - 1) // 2
    copies = [pltpu.make_async_copy(refs[i], refs[count + i], refs[-1].at[i]) for i in range(count)]
    for copy in copies:
        copy.start()
    for copy in copies:
        copy.wait()


def solution(mesh):
    n, npb = mesh.shape["ctx"], mesh.shape["pb"]

    def shards(queries, cache_keys, cache_values, sel_index):
        heads, rows_dev, width = queries.shape[1:]
        rows = heads * rows_dev
        keys = cache_keys.shape[1]
        sel_dev = sel_index.shape[1]
        sel_all, piece, chunk = sel_dev * n, sel_dev // npb, rows // n
        per = max(2, min(n, 256 // chunk))
        while n % per or per % 2:
            per -= 1
        block = per * chunk
        cfg = dict(n=n, npb=npb, per=per, tile=math.gcd(keys, 2048))
        lanes = max(width, chunk)
        pairs = n // 2
        vmem = pl.BlockSpec(memory_space=pltpu.VMEM)
        hbm = pl.BlockSpec(memory_space=pltpu.HBM)
        dma = pltpu.SemaphoreType.DMA
        results = (
            jax.ShapeDtypeStruct((piece, sel_all), f32),
            jax.ShapeDtypeStruct((piece, width), f32),
            jax.ShapeDtypeStruct((n, chunk), f32),
        )
        operands = (queries[0].reshape(rows, width), cache_keys[0], cache_values[0], sel_index)
        parts = pl.pallas_call(
            functools.partial(kernel, cfg),
            out_shape=results,
            in_specs=[hbm] * 4,
            out_specs=(vmem,) * 3,
            scratch_shapes=[
                pltpu.VMEM((rows, width), bf16),
                pltpu.VMEM((keys, width), bf16),
                pltpu.VMEM((keys, width), bf16),
                pltpu.VMEM((1, sel_dev), jnp.int32),
                pltpu.VMEM((width, keys), bf16),
                pltpu.VMEM((keys, block), f32),
                pltpu.VMEM((keys, block), f32),
                pltpu.VMEM((width, block), f32),
                pltpu.VMEM((n, sel_dev, width), bf16),
                pltpu.VMEM((pairs, 2, width, chunk), f32),
                pltpu.VMEM((pairs, 2, width, chunk), i16),
                pltpu.VMEM((pairs, 2, 8, chunk), f32),
                pltpu.VMEM((pairs, width, chunk), i16),
                pltpu.VMEM((pairs, 8, chunk), f32),
                pltpu.VMEM((pairs, width, chunk), i16),
                pltpu.VMEM((pairs, 8, chunk), f32),
                pltpu.VMEM((pairs, width, chunk), i16),
                pltpu.VMEM((pairs, 8, chunk), f32),
                pltpu.VMEM((n, sel_all, chunk), bf16),
                pltpu.VMEM((n, 8, chunk), f32),
                pltpu.VMEM((npb, piece, sel_all), f32),
                pltpu.VMEM((npb, piece, sel_all), f32),
                pltpu.VMEM((npb, n * piece, chunk), bf16),
                pltpu.VMEM((npb, n * piece, chunk), bf16),
                pltpu.VMEM((width, chunk), bf16),
                pltpu.VMEM((npb, width, chunk), bf16),
                pltpu.VMEM((n, piece, width), i16),
                pltpu.VMEM((n, 2, lanes), f32),
                pltpu.VMEM((n, piece, width), i16),
                pltpu.VMEM((n, 2, lanes), f32),
                dma((4,)),
                dma, dma, dma((2,)), dma((2, pairs)), dma((2,)), dma((2,)),
                dma((npb,)), dma((npb,)), dma((npb,)), dma((npb,)), dma((npb,)), dma((npb,)),
                dma((2,)), dma((2,)),
            ],
            compiler_params=pltpu.CompilerParams(
                collective_id=0, has_side_effects=True, vmem_limit_bytes=50 * 1024 * 1024
            ),
        )(*[pltpu.with_memory_space_constraint(a, pltpu.HBM) for a in operands])
        gram, rhs, gap = pl.pallas_call(
            emit,
            out_shape=results,
            in_specs=[vmem] * 3,
            out_specs=(hbm,) * 3,
            scratch_shapes=[dma((3,))],
        )(*[pltpu.with_memory_space_constraint(a, pltpu.VMEM) for a in parts])
        return gram[None], rhs[None], gap.reshape(1, heads, rows_dev)

    in_specs = (
        P("kv", None, "pb", None),
        P("kv", "ctx", None),
        P("kv", "ctx", None),
        P("kv", "ctx"),
    )
    out_specs = (P("kv", ("ctx", "pb"), None), P("kv", ("ctx", "pb"), None), P("kv", None, "pb"))
    return jax.shard_map(shards, mesh=mesh, in_specs=in_specs, out_specs=out_specs, check_vma=False)
```
